32 devices in a mesh: ctx: 4 (over y, core), exp: 8 (over z, x).
Axes of the slice: x: 2, y: 2, z: 4, core: 2. Of those that a mesh axis runs over, the one named last changes fastest.
Arguments:
- queries: bfloat16 [512, 64, 576], P('ctx', 'exp'), may hold values from -1024 to 1024
- latents: bfloat16 [512, 576], P('ctx'), may hold values from -6.1 to 6.1
- block_starts: int32 [8], replicated, may hold values from 0 to 448, as said below
- w_uv: bfloat16 [64, 512, 128], P('exp'), may hold values from -0.25 to 0.25
- moe_tokens: bfloat16 [1024, 7168], P('exp'), may hold values from -6 to 6
- expert_ids: int32 [1024, 2], P('exp'), may hold values from 0 to 7, as said below
- gate_weights: float32 [1024, 2], P('exp'), may hold values from 0.2 to 1
- w_gate: bfloat16 [8, 7168, 512], P('exp', None, 'ctx'), may hold values from -0.0625 to 0.0625
- w_up: bfloat16 [8, 7168, 512], P('exp', None, 'ctx'), may hold values from -0.0625 to 0.0625
- w_down: bfloat16 [8, 512, 7168], P('exp', 'ctx'), may hold values from -0.25 to 0.25
Outputs:
- attended: bfloat16 [512, 64, 128], P('ctx', 'exp')
- moe_out: bfloat16 [1024, 7168], P('exp', 'ctx')
The draws below stay inside these ranges and needn't reach their ends.
Inputs may be any that keep to these rules, and one draw needn't show every extreme that they name: Token t has position block_starts[t // 64] + t % 64; block_starts is a permutation of the multiples of 64 below 512. `expert_ids`: each row names 2 different experts. In the rows of one index of exp, one expert, the same for every index, is named by exactly 48 rows, no expert by more, and the other experts' counts differ by at most one.
All inputs are finite; a program needn't handle non-finite values.
Results may differ from the reference program's by a relative error of at most 0.018.
Values may be sent and summed in bfloat16 or wider, within the bound.
A program may use at most 128 MiB of HBM per device.

```python
import math
import jax
import jax.numpy as jnp
from jax import lax

D = 7168
LAT = 512
ROPE = 64
VDIM = 128
F_DEV = 128
S_DEV = 128
MT_DEV = 128
TOP = 2
HEADS = 64
FF = 512
TOKENS_A = 512
MT_TOK = 1024
EXPERTS = 8
CAP = 48
N_CTX = 4
N_EXP = 8


def block_order(key):
    return jax.random.permutation(jax.random.fold_in(key, 11), 2 * TOKENS_A // S_DEV).astype(jnp.int32)


def draw_block_starts(key, part):
    return (block_order(key) * (S_DEV // 2)).astype(jnp.int32)


def base_latents(key):
    drawn = jax.random.normal(jax.random.fold_in(key, 12), (TOKENS_A, LAT + ROPE), jnp.float32)
    return jnp.clip(drawn, -6.0, 6.0)


def draw_latents(key, part):
    base = base_latents(key)
    return base.astype(jnp.bfloat16)


def draw_queries(key, part):
    base = jax.random.normal(jax.random.fold_in(key, 13), (TOKENS_A, HEADS, LAT + ROPE), jnp.float32)
    base = jnp.clip(base, -6.0, 6.0)
    return base.astype(jnp.bfloat16)


def draw_expert_ids(key, part):
    full = jax.random.randint(jax.random.fold_in(key, 21), (), 0, EXPERTS)
    column = jnp.arange(TOP, dtype=jnp.int32)[None, :]

    def one_block(block_index):
        inner = jax.random.fold_in(key, 100 + block_index)
        ranking = jax.random.permutation(jax.random.fold_in(inner, 1), MT_DEV).astype(jnp.int32)[:, None]
        offset = jax.random.randint(jax.random.fold_in(inner, 2), (), 0, EXPERTS - 1)
        leading = ranking < CAP
        sequence = jnp.where(leading, ranking * (TOP - 1) + column - 1, CAP * (TOP - 1) + (ranking - CAP) * TOP + column)
        others = (sequence + offset) % (EXPERTS - 1)
        others = others + (others >= full).astype(jnp.int32)
        return jnp.where(leading & (column == 0), full, others).astype(jnp.int32)
    blocks = jax.vmap(one_block)(jnp.arange(MT_TOK // MT_DEV, dtype=jnp.int32))
    return blocks.reshape(MT_TOK, TOP).astype(jnp.int32)


def levels(stream_key, extent, shards, least, high):
    def one(axis_at, parts):
        draws = jax.random.uniform(jax.random.fold_in(jax.random.fold_in(stream_key, 6), axis_at), (parts,), jnp.float32, least / len(shards), high / len(shards))
        return jnp.repeat(jnp.exp(draws), extent[axis_at] // parts).reshape((-1,) + (1,) * (len(extent) - axis_at - 1))

    factor_of = one(*shards[0])
    for cut in shards[1:]:
        factor_of = factor_of * one(*cut)
    return factor_of


def noise(key, dims, spread, reach, split=(), held_as=jnp.bfloat16):
    level = levels(key, dims, split, -0.22, 0.18) if split else 1.0
    entries = jax.random.normal(key, dims, jnp.float32) * spread * level
    return jnp.minimum(jnp.maximum(entries, -reach), reach).astype(held_as)


def setup_inputs(seed: int = 0) -> dict:
    splits = jax.random.split(jax.random.key(seed), 11)
    return {
        "queries": draw_queries(jax.random.fold_in(splits[10], 71), 0),
        "latents": draw_latents(jax.random.fold_in(splits[10], 71), 0),
        "block_starts": draw_block_starts(jax.random.fold_in(splits[10], 71), 0),
        "w_uv": noise(splits[3], (HEADS, LAT, VDIM), LAT ** -0.5, 0.25, ((0, 8),)),
        "moe_tokens": noise(splits[4], (MT_TOK, D), 1.0, 6.0, ((0, 8),)),
        "expert_ids": draw_expert_ids(jax.random.fold_in(splits[10], 71), 0),
        "gate_weights": jnp.clip(0.2 + 0.8 * jax.random.uniform(splits[6], (MT_TOK, TOP), jnp.float32) ** levels(splits[6], (MT_TOK, TOP), ((0, 8),), -0.2, 0.2), 0.2, 1.0),
        "w_gate": noise(splits[7], (EXPERTS, D, FF), D ** -0.5, 0.0625, ((0, 8), (2, 4))),
        "w_up": noise(splits[8], (EXPERTS, D, FF), D ** -0.5, 0.0625, ((0, 8), (2, 4))),
        "w_down": noise(splits[9], (EXPERTS, FF, D), FF ** -0.5, 0.25, ((0, 8), (1, 4))),
    }


score_scale = (0.1 * math.log(40.0) + 1.0) ** 2 / math.sqrt(192.0)
neg_fill = -1e+30

def token_positions(block_starts, token_index, half_block):
    block_index = token_index // half_block
    matches = block_index[:, None] == jnp.arange(block_starts.shape[0], dtype=jnp.int32)[None, :]
    first_pos = lax.optimization_barrier(jnp.sum(jnp.where(matches, block_starts[None, :], 0), axis=1))
    return (first_pos + token_index % half_block).astype(jnp.int32)

def slot_targets(expert_ids, expert_count, capacity):
    token_count, picks = expert_ids.shape
    flat_ids = expert_ids.reshape(token_count * picks)
    onehot = (flat_ids[:, None] == jnp.arange(expert_count, dtype=jnp.int32)[None, :]).astype(jnp.int32)
    earlier = jnp.cumsum(onehot, axis=0) - onehot
    slot_index = lax.optimization_barrier(jnp.sum(earlier * onehot, axis=1))
    return (flat_ids * capacity + slot_index).astype(jnp.int32)

def reference(queries, latents, block_starts, w_uv, moe_tokens, expert_ids, gate_weights, w_gate, w_up, w_down):
    positions = token_positions(block_starts, jnp.arange(TOKENS_A, dtype=jnp.int32), S_DEV // 2)
    visible = positions[None, :] <= positions[:, None]
    values = latents[:, :LAT]

    def one_head(pieces):
        head_queries, head_uv = pieces
        scores = jnp.dot(head_queries, latents.T, preferred_element_type=jnp.float32) * score_scale
        masked = jnp.where(visible, scores, neg_fill)
        top_score = lax.optimization_barrier(jnp.max(masked, axis=1, keepdims=True))
        weights = jnp.where(visible, jnp.exp(masked - top_score), 0.0)
        totals = lax.optimization_barrier(jnp.sum(weights, axis=1, keepdims=True))
        blended = jnp.dot(weights.astype(jnp.bfloat16), values, preferred_element_type=jnp.float32)
        latent_out = (blended / totals).astype(jnp.bfloat16)
        return jnp.dot(latent_out, head_uv, preferred_element_type=jnp.float32).astype(jnp.bfloat16)
    per_head = lax.map(one_head, (jnp.transpose(queries, (1, 0, 2)), w_uv))
    attended = jnp.transpose(per_head, (1, 0, 2))
    block_ids = expert_ids.reshape(N_EXP, MT_DEV, TOP)
    targets = jax.vmap(lambda ids: slot_targets(ids, EXPERTS, CAP))(block_ids)
    local_rows = jnp.arange(MT_DEV * TOP, dtype=jnp.int32) // TOP
    global_rows = jnp.arange(N_EXP, dtype=jnp.int32)[:, None] * MT_DEV + local_rows[None, :]

    def fill_block(target_row, token_row, gate_row):
        filled = jnp.zeros((EXPERTS * CAP,), jnp.int32).at[target_row].set(token_row + 1)
        scaled = jnp.zeros((EXPERTS * CAP,), jnp.float32).at[target_row].set(gate_row)
        return (filled, scaled)
    filled, scaled = jax.vmap(fill_block)(targets, global_rows, gate_weights.reshape(N_EXP, MT_DEV * TOP))
    filled = jnp.transpose(filled.reshape(N_EXP, EXPERTS, CAP), (1, 0, 2)).reshape(EXPERTS, N_EXP * CAP)
    scaled = jnp.transpose(scaled.reshape(N_EXP, EXPERTS, CAP), (1, 0, 2)).reshape(EXPERTS, N_EXP * CAP)

    def one_expert(accum, pieces):
        slot_rows, slot_gates, gate_matrix, up_matrix, down_matrix = pieces
        occupied = slot_rows > 0
        source = jnp.where(occupied, slot_rows - 1, 0)
        inputs = jnp.where(occupied[:, None], moe_tokens[source], 0)
        gate_h = jnp.dot(inputs, gate_matrix, preferred_element_type=jnp.float32)
        up_h = jnp.dot(inputs, up_matrix, preferred_element_type=jnp.float32)
        hidden = (jax.nn.silu(gate_h) * up_h).astype(jnp.bfloat16)

        def add_group(group_index, summed):
            begin = (group_index * F_DEV).astype(jnp.int32)
            hidden_part = lax.dynamic_slice_in_dim(hidden, begin, F_DEV, 1)
            down_part = lax.dynamic_slice_in_dim(down_matrix, begin, F_DEV, 0)
            rounded = jnp.dot(hidden_part, down_part, preferred_element_type=jnp.float32).astype(jnp.bfloat16)
            return summed + lax.optimization_barrier(rounded).astype(jnp.float32)
        summed = lax.fori_loop(0, N_CTX, add_group, jnp.zeros((N_EXP * CAP, D), jnp.float32))
        contrib = jnp.where(occupied[:, None], slot_gates[:, None] * summed, 0.0)
        return (accum.at[source].add(contrib), None)
    accum, _ = lax.scan(one_expert, jnp.zeros((MT_TOK, D), jnp.float32), (filled, scaled, w_gate, w_up, w_down))
    return (attended, accum.astype(jnp.bfloat16))
```

```python
import functools
import math

import jax
import jax.numpy as jnp
from jax import lax
from jax.experimental import pallas as pl
from jax.experimental.pallas import tpu as pltpu
from jax.sharding import PartitionSpec as P

score_scale = (0.1 * math.log(40.0) + 1.0) ** 2 / math.sqrt(192.0)
neg_fill = -1e30


def token_positions(block_starts, token_index, half_block):
    block_index = token_index // half_block
    matches = block_index[:, None] == jnp.arange(block_starts.shape[0], dtype=jnp.int32)[None, :]
    first_pos = jnp.sum(jnp.where(matches, block_starts[None, :], 0), axis=1)
    return first_pos + token_index % half_block


def slot_targets(expert_ids, expert_count, capacity):
    token_count, picks = expert_ids.shape
    flat_ids = expert_ids.reshape(token_count * picks)
    onehot = (flat_ids[:, None] == jnp.arange(expert_count, dtype=jnp.int32)[None, :]).astype(
        jnp.int32
    )
    earlier = jnp.cumsum(onehot, axis=0) - onehot
    slot_index = jnp.sum(earlier * onehot, axis=1)
    return flat_ids * capacity + slot_index


def attention(queries, latents, block_starts, w_uv):
    query_tokens, head_count, entry_width = queries.shape
    lat_width = w_uv.shape[1]
    half_block = query_tokens // 2
    row_total = query_tokens * head_count
    flat_queries = queries.reshape(row_total, entry_width)
    own_index = lax.axis_index("ctx") * query_tokens + jnp.arange(query_tokens, dtype=jnp.int32)
    own_positions = token_positions(block_starts, own_index, half_block)
    query_positions = jnp.repeat(own_positions, head_count)
    shard_piece = lax.all_gather(latents, "ctx", axis=0, tiled=True)
    key_positions = token_positions(
        block_starts, jnp.arange(shard_piece.shape[0], dtype=jnp.int32), half_block
    )
    top_score = jnp.full((row_total,), neg_fill, jnp.float32)
    scores = (
        lax.dot_general(
            flat_queries, shard_piece, (((1,), (1,)), ((), ())), preferred_element_type=jnp.float32
        )
        * score_scale
    )
    visible = key_positions[None, :] <= query_positions[:, None]
    masked = jnp.where(visible, scores, neg_fill)
    new_top = jnp.maximum(top_score, jnp.max(masked, axis=1))
    weights = jnp.where(visible, jnp.exp(masked - new_top[:, None]), 0.0)
    totals = jnp.sum(weights, axis=1)
    blended = jnp.dot(
        weights.astype(jnp.bfloat16), shard_piece[:, :lat_width], preferred_element_type=jnp.float32
    )
    top_score, totals, blended = (new_top, totals, blended)
    latent_out = (
        (blended / totals[:, None])
        .astype(jnp.bfloat16)
        .reshape(query_tokens, head_count, lat_width)
    )
    attended = jnp.einsum(
        "shl,hlv->shv", latent_out, w_uv, preferred_element_type=jnp.float32
    ).astype(jnp.bfloat16)
    return attended


def routed_plain(moe_tokens, expert_ids, gate_weights, w_gate, w_up, w_down):
    token_count, picks = expert_ids.shape
    model_width = moe_tokens.shape[1]
    expert_count = lax.axis_size("exp")
    capacity = 3 * token_count * picks // (2 * expert_count)
    targets = slot_targets(expert_ids, expert_count, capacity)
    source_row = jnp.arange(token_count * picks, dtype=jnp.int32) // picks
    filled = jnp.zeros((expert_count * capacity,), jnp.int32).at[targets].set(source_row + 1)
    occupied = filled > 0
    gate_matrix = w_gate[0]
    up_matrix = w_up[0]
    down_matrix = w_down[0]
    picked_rows = moe_tokens[jnp.where(occupied, filled - 1, 0)]
    outgoing = jnp.where(occupied[:, None], picked_rows, 0).reshape(
        expert_count, capacity, model_width
    )
    arrived = lax.all_to_all(outgoing, "exp", split_axis=0, concat_axis=0, tiled=True)
    senders, slot_count, width_in = arrived.shape
    flat_rows = arrived.reshape(senders * slot_count, width_in)
    gate_h = jnp.dot(flat_rows, gate_matrix, preferred_element_type=jnp.float32)
    up_h = jnp.dot(flat_rows, up_matrix, preferred_element_type=jnp.float32)
    hidden = (jax.nn.silu(gate_h) * up_h).astype(jnp.bfloat16)
    rounded = jnp.dot(hidden, down_matrix, preferred_element_type=jnp.float32).astype(jnp.bfloat16)
    rounded = lax.optimization_barrier(rounded.reshape(senders, slot_count, width_in))
    summed = lax.psum_scatter(
        rounded.astype(jnp.float32).astype(jnp.bfloat16), "ctx", scatter_dimension=2, tiled=True
    ).astype(jnp.float32)
    returned = lax.all_to_all(
        summed.astype(jnp.bfloat16), "exp", split_axis=0, concat_axis=0, tiled=True
    ).astype(summed.dtype)
    out_width = returned.shape[2]
    gathered = returned.reshape(expert_count * capacity, out_width)[targets].reshape(
        token_count, picks, out_width
    )
    weighted = jnp.sum(gathered * gate_weights[:, :, None], axis=1)
    return weighted.astype(jnp.bfloat16)


def flip_bits(index, bits):
    flipped = index
    for bit in range(bits.bit_length()):
        if (bits >> bit) % 2:
            flipped = flipped + (1 << bit) * (1 - 2 * ((index // (1 << bit)) % 2))
    return flipped


def step_order(count):
    half = count // 2
    near, far = list(range(1, half)), list(range(half, count))
    order = []
    for at in range(half):
        if at < len(near):
            order.append(near[at])
        order.append(far[at])
    return order


def dot_f32(left, right):
    return jnp.dot(left, right, preferred_element_type=jnp.float32)


def routed_kernel(
    count, outgoing, own_rows, combine, gate_hbm, up_hbm, down_hbm, out_ref,
    gate_w, up_w, down_w, arrived, kept, core_send, core_recv, row_send, row_recv,
    back_send, returned, load_sem, own_sem,
    out_s, out_r, side_s, side_r, near_s, near_r, relay_s, relay_r,
    core_s, core_r, row_s, row_r, back_s, back_r,
):
    me = lax.axis_index("exp")
    ctx = lax.axis_index("ctx")
    core = ctx % 2
    other_core = ctx + 1 - 2 * core
    other_row = (ctx + 2) % 4
    width = outgoing.shape[2]

    loads = [
        pltpu.make_async_copy(gate_hbm.at[0], gate_w, load_sem.at[0]),
        pltpu.make_async_copy(up_hbm.at[0], up_w, load_sem.at[1]),
        pltpu.make_async_copy(down_hbm.at[0], down_w, load_sem.at[2]),
    ]
    for load in loads:
        load.start()

    barrier = pltpu.get_barrier_semaphore()
    for k in range(1, count):
        pl.semaphore_signal(
            barrier, inc=1, device_id={"exp": flip_bits(me, k), "ctx": ctx},
            device_id_type=pl.DeviceIdType.MESH,
        )
    for peer in (other_core, other_row):
        pl.semaphore_signal(
            barrier, inc=1, device_id={"exp": me, "ctx": peer},
            device_id_type=pl.DeviceIdType.MESH,
        )
    pl.semaphore_wait(barrier, count + 1)

    def remote(source, target, send, recv, exp, ctx_at):
        return pltpu.make_async_remote_copy(
            src_ref=source, dst_ref=target, send_sem=send, recv_sem=recv,
            device_id={"exp": exp, "ctx": ctx_at}, device_id_type=pl.DeviceIdType.MESH,
        )

    def dispatch(k):
        to = flip_bits(me, k)
        return remote(
            outgoing.at[to], arrived.at[ctx, me], out_s.at[k], out_r.at[k], to, ctx
        )

    def across(k):
        block = arrived.at[ctx, flip_bits(me, k)]
        return remote(block, block, side_s.at[k], side_r.at[k], me, other_row)

    def beside(k):
        block = arrived.at[ctx, flip_bits(me, k)]
        return remote(block, block, near_s.at[k], near_r.at[k], me, other_core)

    def relay(k):
        block = arrived.at[other_row, flip_bits(me, k)]
        return remote(block, block, relay_s.at[k], relay_r.at[k], me, other_core)

    def core_swap(k):
        return remote(
            core_send.at[k], core_recv.at[k], core_s.at[k], core_r.at[k], me, other_core
        )

    def row_swap(k):
        return remote(
            row_send.at[k], row_recv.at[k], row_s.at[k], row_r.at[k], me, other_row
        )

    def give_back(k):
        to = flip_bits(me, k)
        return remote(
            back_send.at[k], returned.at[me], back_s.at[k], back_r.at[k], to, ctx
        )

    order = step_order(count)
    for k in order:
        dispatch(k).start()

    def columns(at):
        return pl.ds(pl.multiple_of(at * width, 128), width)

    def experts(k):
        at = flip_bits(me, k)
        rows = outgoing.shape[1]
        gate_h = jnp.zeros((rows, gate_w.shape[1]), jnp.float32)
        up_h = jnp.zeros((rows, up_w.shape[1]), jnp.float32)
        for quarter in range(4):
            span = pl.ds(quarter * width, width)
            block = own_rows[:, span] if k == 0 else arrived[quarter, at]
            gate_h += dot_f32(block, gate_w[span, :])
            up_h += dot_f32(block, up_w[span, :])
        hidden = (gate_h / (1.0 + jnp.exp(-gate_h)) * up_h).astype(jnp.bfloat16)
        mate = 1 - core
        for side in range(2):
            core_send[k, side] = dot_f32(hidden, down_w[:, columns(mate + 2 * side)]).astype(
                jnp.bfloat16
            )
        core_swap(k).start()
        for side in range(2):
            kept[k, side] = dot_f32(hidden, down_w[:, columns(core + 2 * side)]).astype(
                jnp.bfloat16
            )

    def pair_sum(k, side):
        return kept[k, side].astype(jnp.float32) + core_recv[k, side].astype(jnp.float32)

    def forward(k):
        if k:
            dispatch(k).wait_recv()
            across(k).start()
            beside(k).start()

    def pass_on(k):
        if k:
            across(k).wait_recv()
            relay(k).start()

    def compute(k):
        if k:
            beside(k).wait_recv()
            relay(k).wait_recv()
        experts(k)

    def sum_cores(k):
        core_swap(k).wait_recv()
        row_send[k] = pair_sum(k, 1 - ctx // 2).astype(jnp.bfloat16)
        row_swap(k).start()

    def sum_rows(k):
        row_swap(k).wait_recv()
        total = pair_sum(k, ctx // 2) + row_recv[k].astype(jnp.float32)
        if k:
            back_send[k] = total.astype(jnp.bfloat16)
            give_back(k).start()
        else:
            returned[me] = total.astype(jnp.bfloat16)

    for load in loads:
        load.wait()
    steps = [0] + order
    lags = ((forward, 0), (pass_on, 1), (compute, 2), (sum_cores, 3), (sum_rows, 5))
    for at in range(len(steps) + 5):
        for stage, lag in lags:
            if 0 <= at - lag < len(steps):
                stage(steps[at - lag])

    for k in order:
        give_back(k).wait_recv()
    back = returned[...].reshape(combine.shape[1], width)
    high = combine[...].astype(jnp.bfloat16)
    low = (combine[...] - high.astype(jnp.float32)).astype(jnp.bfloat16)
    out_ref[...] = (dot_f32(high, back) + dot_f32(low, back)).astype(jnp.bfloat16)
    for k in steps:
        core_swap(k).wait_send()
        row_swap(k).wait_send()
        if k:
            for copy in (dispatch, across, beside, relay, give_back):
                copy(k).wait_send()


def routed_fused(moe_tokens, expert_ids, gate_weights, w_gate, w_up, w_down):
    token_count, picks = expert_ids.shape
    model_width = moe_tokens.shape[1]
    hidden_width = w_gate.shape[2]
    count = lax.axis_size("exp")
    width = model_width // lax.axis_size("ctx")
    capacity = 3 * token_count * picks // (2 * count)
    targets = slot_targets(expert_ids, count, capacity).reshape(token_count, picks)
    slots = jnp.arange(count * capacity, dtype=jnp.int32)
    chosen = jnp.zeros((count * capacity, token_count), jnp.bool_)
    combine = jnp.zeros((token_count, count * capacity), jnp.float32)
    for pick in range(picks):
        chosen = chosen | (slots[:, None] == targets[None, :, pick])
        combine = combine + jnp.where(
            slots[None, :] == targets[:, pick : pick + 1], gate_weights[:, pick : pick + 1], 0.0
        )
    chosen = chosen.astype(jnp.bfloat16)
    quarter = lax.dynamic_slice_in_dim(moe_tokens, lax.axis_index("ctx") * width, width, 1)
    outgoing = jnp.dot(chosen, quarter, preferred_element_type=jnp.float32)
    outgoing = outgoing.astype(jnp.bfloat16).reshape(count, capacity, width)
    mine = lax.dynamic_slice_in_dim(chosen, lax.axis_index("exp") * capacity, capacity, 0)
    own_rows = jnp.dot(mine, moe_tokens, preferred_element_type=jnp.float32).astype(jnp.bfloat16)
    vmem = pl.BlockSpec(memory_space=pltpu.VMEM)
    hbm = pl.BlockSpec(memory_space=pl.ANY)
    block = (capacity, width)
    dtype = jnp.bfloat16
    return pl.pallas_call(
        functools.partial(routed_kernel, count),
        out_shape=jax.ShapeDtypeStruct((token_count, width), dtype),
        in_specs=[vmem, vmem, vmem, hbm, hbm, hbm],
        out_specs=vmem,
        scratch_shapes=[
            pltpu.VMEM((model_width, hidden_width), dtype),
            pltpu.VMEM((model_width, hidden_width), dtype),
            pltpu.VMEM((hidden_width, model_width), dtype),
            pltpu.VMEM((4, count) + block, dtype),
            pltpu.VMEM((count, 2) + block, dtype),
            pltpu.VMEM((count, 2) + block, dtype),
            pltpu.VMEM((count, 2) + block, dtype),
            pltpu.VMEM((count,) + block, dtype),
            pltpu.VMEM((count,) + block, dtype),
            pltpu.VMEM((count,) + block, dtype),
            pltpu.VMEM((count,) + block, dtype),
            pltpu.SemaphoreType.DMA((3,)),
            pltpu.SemaphoreType.DMA((1,)),
        ]
        + [pltpu.SemaphoreType.DMA((count,))] * 14,
        compiler_params=pltpu.CompilerParams(
            collective_id=0, has_side_effects=True, vmem_limit_bytes=56 * 1024 * 1024
        ),
    )(outgoing, own_rows, combine, w_gate, w_up, w_down)


def shards(
    queries, latents, block_starts, w_uv, moe_tokens, expert_ids, gate_weights, w_gate, w_up, w_down
):
    attended = attention(queries, latents, block_starts, w_uv)
    count = lax.axis_size("exp")
    ways = lax.axis_size("ctx")
    capacity = 3 * expert_ids.shape[0] * expert_ids.shape[1] // (2 * count)
    fits = ways == 4 and count & (count - 1) == 0 and count >= 4 and capacity % 16 == 0
    routed = routed_fused if fits and moe_tokens.shape[1] % (128 * ways) == 0 else routed_plain
    return attended, routed(moe_tokens, expert_ids, gate_weights, w_gate, w_up, w_down)


def solution(mesh):
    in_specs = (
        P("ctx", "exp", None),
        P("ctx", None),
        P(),
        P("exp", None, None),
        P("exp", None),
        P("exp", None),
        P("exp", None),
        P("exp", None, "ctx"),
        P("exp", None, "ctx"),
        P("exp", "ctx", None),
    )
    out_specs = (P("ctx", "exp", None), P("exp", "ctx"))
    return jax.shard_map(shards, mesh=mesh, in_specs=in_specs, out_specs=out_specs, check_vma=False)
```

```python
import functools
import math

import jax
import jax.numpy as jnp
from jax import lax
from jax.experimental import pallas as pl
from jax.experimental.pallas import tpu as pltpu
from jax.sharding import PartitionSpec as P

score_scale = (0.1 * math.log(40.0) + 1.0) ** 2 / math.sqrt(192.0)
neg_fill = -1e30


def token_positions(block_starts, token_index, half_block):
    block_index = token_index // half_block
    matches = block_index[:, None] == jnp.arange(block_starts.shape[0], dtype=jnp.int32)[None, :]
    first_pos = jnp.sum(jnp.where(matches, block_starts[None, :], 0), axis=1)
    return first_pos + token_index % half_block


def slot_targets(expert_ids, expert_count, capacity):
    token_count, picks = expert_ids.shape
    flat_ids = expert_ids.reshape(token_count * picks)
    onehot = (flat_ids[:, None] == jnp.arange(expert_count, dtype=jnp.int32)[None, :]).astype(
        jnp.int32
    )
    earlier = jnp.cumsum(onehot, axis=0) - onehot
    slot_index = jnp.sum(earlier * onehot, axis=1)
    return flat_ids * capacity + slot_index


def attention(queries, latents, block_starts, w_uv):
    query_tokens, head_count, entry_width = queries.shape
    lat_width = w_uv.shape[1]
    half_block = query_tokens // 2
    row_total = query_tokens * head_count
    flat_queries = queries.reshape(row_total, entry_width)
    own_index = lax.axis_index("ctx") * query_tokens + jnp.arange(query_tokens, dtype=jnp.int32)
    own_positions = token_positions(block_starts, own_index, half_block)
    query_positions = jnp.repeat(own_positions, head_count)
    shard_piece = lax.all_gather(latents, "ctx", axis=0, tiled=True)
    key_positions = token_positions(
        block_starts, jnp.arange(shard_piece.shape[0], dtype=jnp.int32), half_block
    )
    top_score = jnp.full((row_total,), neg_fill, jnp.float32)
    scores = (
        lax.dot_general(
            flat_queries, shard_piece, (((1,), (1,)), ((), ())), preferred_element_type=jnp.float32
        )
        * score_scale
    )
    visible = key_positions[None, :] <= query_positions[:, None]
    masked = jnp.where(visible, scores, neg_fill)
    new_top = jnp.maximum(top_score, jnp.max(masked, axis=1))
    weights = jnp.where(visible, jnp.exp(masked - new_top[:, None]), 0.0)
    totals = jnp.sum(weights, axis=1)
    blended = jnp.dot(
        weights.astype(jnp.bfloat16), shard_piece[:, :lat_width], preferred_element_type=jnp.float32
    )
    top_score, totals, blended = (new_top, totals, blended)
    latent_out = (
        (blended / totals[:, None])
        .astype(jnp.bfloat16)
        .reshape(query_tokens, head_count, lat_width)
    )
    attended = jnp.einsum(
        "shl,hlv->shv", latent_out, w_uv, preferred_element_type=jnp.float32
    ).astype(jnp.bfloat16)
    return attended


def routed_plain(moe_tokens, expert_ids, gate_weights, w_gate, w_up, w_down):
    token_count, picks = expert_ids.shape
    model_width = moe_tokens.shape[1]
    expert_count = lax.axis_size("exp")
    capacity = 3 * token_count * picks // (2 * expert_count)
    targets = slot_targets(expert_ids, expert_count, capacity)
    source_row = jnp.arange(token_count * picks, dtype=jnp.int32) // picks
    filled = jnp.zeros((expert_count * capacity,), jnp.int32).at[targets].set(source_row + 1)
    occupied = filled > 0
    gate_matrix = w_gate[0]
    up_matrix = w_up[0]
    down_matrix = w_down[0]
    picked_rows = moe_tokens[jnp.where(occupied, filled - 1, 0)]
    outgoing = jnp.where(occupied[:, None], picked_rows, 0).reshape(
        expert_count, capacity, model_width
    )
    arrived = lax.all_to_all(outgoing, "exp", split_axis=0, concat_axis=0, tiled=True)
    senders, slot_count, width_in = arrived.shape
    flat_rows = arrived.reshape(senders * slot_count, width_in)
    gate_h = jnp.dot(flat_rows, gate_matrix, preferred_element_type=jnp.float32)
    up_h = jnp.dot(flat_rows, up_matrix, preferred_element_type=jnp.float32)
    hidden = (jax.nn.silu(gate_h) * up_h).astype(jnp.bfloat16)
    rounded = jnp.dot(hidden, down_matrix, preferred_element_type=jnp.float32).astype(jnp.bfloat16)
    rounded = lax.optimization_barrier(rounded.reshape(senders, slot_count, width_in))
    summed = lax.psum_scatter(
        rounded.astype(jnp.float32).astype(jnp.bfloat16), "ctx", scatter_dimension=2, tiled=True
    ).astype(jnp.float32)
    returned = lax.all_to_all(
        summed.astype(jnp.bfloat16), "exp", split_axis=0, concat_axis=0, tiled=True
    ).astype(summed.dtype)
    out_width = returned.shape[2]
    gathered = returned.reshape(expert_count * capacity, out_width)[targets].reshape(
        token_count, picks, out_width
    )
    weighted = jnp.sum(gathered * gate_weights[:, :, None], axis=1)
    return weighted.astype(jnp.bfloat16)


def flip_bits(index, bits):
    flipped = index
    for bit in range(bits.bit_length()):
        if (bits >> bit) % 2:
            flipped = flipped + (1 << bit) * (1 - 2 * ((index // (1 << bit)) % 2))
    return flipped


def plan(count, heads):
    half = count // 2
    near, far = list(range(1, half)), list(range(half, count))
    left = list(range(heads))
    order = [("forward", near[0]), ("compute", 0)]
    order += [("forward", k) for k in near[1:]]
    order += [("pass_on", near[0]), ("sum_cores", 0), ("latents", 0)]
    for at, k in enumerate(near):
        order += [("attend", left.pop(0)) for _ in range(min(1, len(left)))]
        if at + 1 < len(near):
            order += [("pass_on", near[at + 1])]
        order += [("compute", k)]
        if at:
            order += [("sum_cores", near[at - 1])]
        else:
            order += [("sum_rows", 0)]
    order += [("forward", far[0]), ("sum_cores", near[-1])]
    for at, k in enumerate(far):
        if at:
            order += [("forward", k), ("sum_cores", far[at - 1])]
        if at < len(near):
            order += [("sum_rows", near[at])]
        share = -(-len(left) // max(1, len(far) - 1 - at))
        order += [("attend", left.pop(0)) for _ in range(min(share, len(left)))]
        order += [("pass_on", k)]
        if at:
            order += [("sum_rows", far[at - 1])]
        order += [("compute", k)]
    return order + [("sum_cores", far[-1]), ("sum_rows", far[-1])]


def dot_first(left, right):
    return lax.dot_general(
        left, right, (((0,), (0,)), ((), ())), preferred_element_type=jnp.float32
    )


def dot_f32(left, right):
    return jnp.dot(left, right, preferred_element_type=jnp.float32)


def routed_kernel(
    count, outgoing, own_rows, combine, latents, starts, gate_hbm, up_hbm, down_hbm,
    queries_hbm, uv_hbm, out_ref, attended_ref,
    gate_w, up_w, down_w, query_t, uv_w, every_latent, value_t, seen, arrived, kept, core_send, core_recv, row_send, row_recv,
    back_send, returned, load_sem, lat_s, lat_r,
    out_s, out_r, side_s, side_r, near_s, near_r, relay_s, relay_r,
    core_s, core_r, row_s, row_r, back_s, back_r,
):
    me = lax.axis_index("exp")
    ctx = lax.axis_index("ctx")
    core = ctx % 2
    other_core = ctx + 1 - 2 * core
    other_row = (ctx + 2) % 4
    width = outgoing.shape[2]

    loads = [
        pltpu.make_async_copy(gate_hbm.at[0], gate_w, load_sem.at[0]),
        pltpu.make_async_copy(up_hbm.at[0], up_w, load_sem.at[1]),
        pltpu.make_async_copy(down_hbm.at[0], down_w, load_sem.at[2]),
        pltpu.make_async_copy(queries_hbm, query_t, load_sem.at[3]),
        pltpu.make_async_copy(uv_hbm, uv_w, load_sem.at[4]),
    ]
    for load in loads:
        load.start()

    barrier = pltpu.get_barrier_semaphore()
    for k in range(1, count):
        pl.semaphore_signal(
            barrier, inc=1, device_id={"exp": flip_bits(me, k), "ctx": ctx},
            device_id_type=pl.DeviceIdType.MESH,
        )
    for peer in (other_core, other_row):
        pl.semaphore_signal(
            barrier, inc=1, device_id={"exp": me, "ctx": peer},
            device_id_type=pl.DeviceIdType.MESH,
        )
    pl.semaphore_wait(barrier, count + 1)

    def remote(source, target, send, recv, exp, ctx_at):
        return pltpu.make_async_remote_copy(
            src_ref=source, dst_ref=target, send_sem=send, recv_sem=recv,
            device_id={"exp": exp, "ctx": ctx_at}, device_id_type=pl.DeviceIdType.MESH,
        )

    def dispatch(k):
        to = flip_bits(me, k)
        return remote(
            outgoing.at[to], arrived.at[ctx, me], out_s.at[k], out_r.at[k], to, ctx
        )

    def across(k):
        block = arrived.at[ctx, flip_bits(me, k)]
        return remote(block, block, side_s.at[k], side_r.at[k], me, other_row)

    def beside(k):
        block = arrived.at[ctx, flip_bits(me, k)]
        return remote(block, block, near_s.at[k], near_r.at[k], me, other_core)

    def relay(k):
        block = arrived.at[other_row, flip_bits(me, k)]
        return remote(block, block, relay_s.at[k], relay_r.at[k], me, other_core)

    def core_swap(k):
        return remote(
            core_send.at[k], core_recv.at[k], core_s.at[k], core_r.at[k], me, other_core
        )

    def row_swap(k):
        return remote(
            row_send.at[k], row_recv.at[k], row_s.at[k], row_r.at[k], me, other_row
        )

    def give_back(k):
        to = flip_bits(me, k)
        return remote(
            back_send.at[k], returned.at[me], back_s.at[k], back_r.at[k], to, ctx
        )

    def own_latents(step, peer):
        return remote(
            latents, every_latent.at[ctx], lat_s.at[step], lat_r.at[step], me, peer
        )

    row_block = every_latent.at[other_row]
    latents_beside = own_latents(0, other_core)
    latents_across = own_latents(1, other_row)
    latents_relay = remote(row_block, row_block, lat_s.at[2], lat_r.at[2], me, other_core)
    latents_across.start()
    latents_beside.start()
    partners = list(range(1, count))
    for k in partners:
        dispatch(k).start()
    every_latent[ctx] = latents[...]

    tokens = latents.shape[0]
    half_block = tokens // 2
    lat_width = uv_w.shape[1]

    def gather_latents(_):
        latents_across.wait_recv()
        latents_relay.start()
        key_at = lax.broadcasted_iota(jnp.int32, (4 * tokens, tokens), 0)
        own_at = lax.broadcasted_iota(jnp.int32, (4 * tokens, tokens), 1)
        key_block = key_at // half_block
        key_start = jnp.zeros_like(key_at)
        for block in range(8):
            key_start = jnp.where(key_block == block, starts[block], key_start)
        own_start = jnp.where(own_at < half_block, starts[2 * ctx], starts[2 * ctx + 1])
        key_position = key_start + key_at % half_block
        seen[...] = (key_position <= own_start + own_at % half_block).astype(jnp.float32)
        latents_beside.wait_recv()
        latents_relay.wait_recv()
        for block in range(4):
            value_t[:, pl.ds(block * tokens, tokens)] = every_latent[block, :, :lat_width].T

    def attend(head):
        keys = every_latent[...].reshape(4 * tokens, latents.shape[1])
        scores = dot_f32(keys, query_t[head]) * score_scale
        visible = seen[...] > 0.5
        masked = jnp.where(visible, scores, neg_fill)
        top = jnp.max(masked, axis=0, keepdims=True)
        weights = jnp.where(visible, jnp.exp(masked - top), 0.0)
        totals = jnp.sum(weights, axis=0, keepdims=True)
        blended = dot_f32(value_t[...], weights.astype(jnp.bfloat16))
        latent_out = (blended / totals).astype(jnp.bfloat16)
        attended_ref[head] = dot_first(latent_out, uv_w[head]).astype(jnp.bfloat16)

    def columns(at):
        return pl.ds(pl.multiple_of(at * width, 128), width)

    def experts(k):
        at = flip_bits(me, k)
        rows = outgoing.shape[1]
        gate_h = jnp.zeros((rows, gate_w.shape[1]), jnp.float32)
        up_h = jnp.zeros((rows, up_w.shape[1]), jnp.float32)
        for quarter in range(4):
            span = pl.ds(quarter * width, width)
            block = own_rows[:, span] if k == 0 else arrived[quarter, at]
            gate_h += dot_f32(block, gate_w[span, :])
            up_h += dot_f32(block, up_w[span, :])
        hidden = (gate_h / (1.0 + jnp.exp(-gate_h)) * up_h).astype(jnp.bfloat16)
        mate = 1 - core
        for side in range(2):
            core_send[k, side] = dot_f32(hidden, down_w[:, columns(mate + 2 * side)]).astype(
                jnp.bfloat16
            )
        core_swap(k).start()
        for side in range(2):
            kept[k, side] = dot_f32(hidden, down_w[:, columns(core + 2 * side)]).astype(
                jnp.bfloat16
            )

    def pair_sum(k, side):
        return kept[k, side].astype(jnp.float32) + core_recv[k, side].astype(jnp.float32)

    def forward(k):
        if k:
            dispatch(k).wait_recv()
            across(k).start()
            beside(k).start()

    def pass_on(k):
        if k:
            across(k).wait_recv()
            relay(k).start()

    def compute(k):
        if k:
            beside(k).wait_recv()
            relay(k).wait_recv()
        experts(k)

    def sum_cores(k):
        core_swap(k).wait_recv()
        row_send[k] = pair_sum(k, 1 - ctx // 2).astype(jnp.bfloat16)
        row_swap(k).start()

    def sum_rows(k):
        row_swap(k).wait_recv()
        total = pair_sum(k, ctx // 2) + row_recv[k].astype(jnp.float32)
        if k:
            back_send[k] = total.astype(jnp.bfloat16)
            give_back(k).start()
        else:
            returned[me] = total.astype(jnp.bfloat16)

    stages = {
        "forward": forward, "pass_on": pass_on, "compute": compute, "sum_cores": sum_cores,
        "sum_rows": sum_rows, "attend": attend, "latents": gather_latents,
    }
    waiting = list(loads)
    for stage, at in plan(count, query_t.shape[0]):
        if stage == "compute":
            while waiting:
                waiting.pop(0).wait()
        stages[stage](at)

    for k in partners:
        give_back(k).wait_recv()
    back = returned[...].reshape(combine.shape[1], width)
    high = combine[...].astype(jnp.bfloat16)
    low = (combine[...] - high.astype(jnp.float32)).astype(jnp.bfloat16)
    out_ref[...] = (dot_f32(high, back) + dot_f32(low, back)).astype(jnp.bfloat16)
    for copy in (latents_across, latents_beside, latents_relay):
        copy.wait_send()
    for k in [0] + partners:
        core_swap(k).wait_send()
        row_swap(k).wait_send()
        if k:
            for copy in (dispatch, across, beside, relay, give_back):
                copy(k).wait_send()


def window_fused(
    queries, latents, block_starts, w_uv, moe_tokens, expert_ids, gate_weights, w_gate, w_up, w_down
):
    queries = jnp.transpose(queries, (1, 2, 0))
    heads, entry_width, query_tokens = queries.shape
    lat_width, value_width = w_uv.shape[1:]
    key_count = lax.axis_size("ctx") * query_tokens
    token_count, picks = expert_ids.shape
    model_width = moe_tokens.shape[1]
    hidden_width = w_gate.shape[2]
    count = lax.axis_size("exp")
    width = model_width // lax.axis_size("ctx")
    capacity = 3 * token_count * picks // (2 * count)
    targets = slot_targets(expert_ids, count, capacity).reshape(token_count, picks)
    slots = jnp.arange(count * capacity, dtype=jnp.int32)
    chosen = jnp.zeros((count * capacity, token_count), jnp.bool_)
    combine = jnp.zeros((token_count, count * capacity), jnp.float32)
    for pick in range(picks):
        chosen = chosen | (slots[:, None] == targets[None, :, pick])
        combine = combine + jnp.where(
            slots[None, :] == targets[:, pick : pick + 1], gate_weights[:, pick : pick + 1], 0.0
        )
    chosen = chosen.astype(jnp.bfloat16)
    quarter = lax.dynamic_slice_in_dim(moe_tokens, lax.axis_index("ctx") * width, width, 1)
    outgoing = jnp.dot(chosen, quarter, preferred_element_type=jnp.float32)
    outgoing = outgoing.astype(jnp.bfloat16).reshape(count, capacity, width)
    mine = lax.dynamic_slice_in_dim(chosen, lax.axis_index("exp") * capacity, capacity, 0)
    own_rows = jnp.dot(mine, moe_tokens, preferred_element_type=jnp.float32).astype(jnp.bfloat16)
    vmem = pl.BlockSpec(memory_space=pltpu.VMEM)
    hbm = pl.BlockSpec(memory_space=pl.ANY)
    block = (capacity, width)
    dtype = jnp.bfloat16
    routed, attended = pl.pallas_call(
        functools.partial(routed_kernel, count),
        out_shape=(
            jax.ShapeDtypeStruct((token_count, width), dtype),
            jax.ShapeDtypeStruct((heads, query_tokens, value_width), dtype),
        ),
        in_specs=[vmem] * 4 + [pl.BlockSpec(memory_space=pltpu.SMEM)] + [hbm] * 5,
        out_specs=(vmem, vmem),
        scratch_shapes=[
            pltpu.VMEM((model_width, hidden_width), dtype),
            pltpu.VMEM((model_width, hidden_width), dtype),
            pltpu.VMEM((hidden_width, model_width), dtype),
            pltpu.VMEM(queries.shape, dtype),
            pltpu.VMEM(w_uv.shape, dtype),
            pltpu.VMEM((4,) + latents.shape, dtype),
            pltpu.VMEM((lat_width, key_count), dtype),
            pltpu.VMEM((key_count, query_tokens), jnp.float32),
            pltpu.VMEM((4, count) + block, dtype),
            pltpu.VMEM((count, 2) + block, dtype),
            pltpu.VMEM((count, 2) + block, dtype),
            pltpu.VMEM((count, 2) + block, dtype),
            pltpu.VMEM((count,) + block, dtype),
            pltpu.VMEM((count,) + block, dtype),
            pltpu.VMEM((count,) + block, dtype),
            pltpu.VMEM((count,) + block, dtype),
            pltpu.SemaphoreType.DMA((5,)),
            pltpu.SemaphoreType.DMA((3,)),
            pltpu.SemaphoreType.DMA((3,)),
        ]
        + [pltpu.SemaphoreType.DMA((count,))] * 14,
        compiler_params=pltpu.CompilerParams(
            collective_id=0, has_side_effects=True, vmem_limit_bytes=56 * 1024 * 1024
        ),
    )(
        outgoing, own_rows, combine, latents, block_starts, w_gate, w_up, w_down, queries, w_uv
    )
    return jnp.transpose(attended, (1, 0, 2)), routed


def shards(
    queries, latents, block_starts, w_uv, moe_tokens, expert_ids, gate_weights, w_gate, w_up, w_down
):
    count = lax.axis_size("exp")
    ways = lax.axis_size("ctx")
    token_count, picks = expert_ids.shape
    capacity = 3 * token_count * picks // (2 * count)
    fits = ways == 4 and count & (count - 1) == 0 and count >= 4 and capacity % 16 == 0
    fits = fits and moe_tokens.shape[1] % (128 * ways) == 0 and block_starts.shape[0] == 8
    if fits:
        return window_fused(
            queries, latents, block_starts, w_uv, moe_tokens, expert_ids, gate_weights,
            w_gate, w_up, w_down,
        )
    attended = attention(queries, latents, block_starts, w_uv)
    return attended, routed_plain(moe_tokens, expert_ids, gate_weights, w_gate, w_up, w_down)


def solution(mesh):
    in_specs = (
        P("ctx", "exp", None),
        P("ctx", None),
        P(),
        P("exp", None, None),
        P("exp", None),
        P("exp", None),
        P("exp", None),
        P("exp", None, "ctx"),
        P("exp", None, "ctx"),
        P("exp", "ctx", None),
    )
    out_specs = (P("ctx", "exp", None), P("exp", "ctx"))
    return jax.shard_map(shards, mesh=mesh, in_specs=in_specs, out_specs=out_specs, check_vma=False)
```
